32 devices in a mesh: blk: 8 (over z, x), dp: 4 (over y, core).
Axes of the slice: x: 2, y: 2, z: 4, core: 2. Of those that a mesh axis runs over, the one named last changes fastest.
Arguments:
- tokens: bfloat16 [4096, 3072], P(('blk', 'dp')), may hold values from -6 to 6
- expert_ids: int32 [4096, 2], P(('blk', 'dp')), may hold values from 0 to 7, as said below
- gate_num: int32 [4096], P(('blk', 'dp')), may hold values from 1 to 255
- gate_weight: bfloat16 [3072, 8192], P('dp', 'blk'), may hold values from -0.109375 to 0.109375
- up_weight: bfloat16 [3072, 8192], P('dp', 'blk'), may hold values from -0.109375 to 0.109375
- down_weight: bfloat16 [8192, 3072], P(('blk', 'dp')), may hold values from -0.0625 to 0.0625
Outputs:
- moe_out: bfloat16 [4096, 3072], P(('blk', 'dp'))
The draws below stay inside these ranges and needn't reach their ends.
Inputs may be any that keep to these rules, and one draw needn't show every extreme that they name: `expert_ids`: each row names two different experts. Among the 128 rows of one device (aligned blocks), between 1 and 64 name expert 0, and in every draw the rows of some device include exactly 64 such rows.
All inputs are finite; a program needn't handle non-finite values.
Results may differ from the reference program's by a relative error of at most 0.018.
Values may be sent and summed in bfloat16 or wider, within the bound.
A program may use at most 192 MiB of HBM per device.

```python
import jax
import jax.numpy as jnp
from jax import lax

D = 3072
FF = 8192
EXPERTS = 8
T_DEV = 128
CAP = 64
TOKENS = 4096
N_BLK = 8
N_DP = 4


def draw_expert_ids(key, part):
    blocks = TOKENS // T_DEV
    keys = jax.random.split(jax.random.fold_in(key, 11), 6)
    loads = jax.random.randint(keys[0], (blocks,), 1, CAP + 1)
    fullest = jax.random.randint(keys[1], (), 0, blocks)
    loads = jnp.where(jnp.arange(blocks) == fullest, CAP, loads)
    scores = jax.random.randint(keys[2], (blocks, T_DEV), 0, 1 << 20) * T_DEV + jnp.arange(T_DEV)[None, :]
    ranks = jnp.argsort(jnp.argsort(scores, axis=1), axis=1)
    chosen = ranks < loads[:, None]
    other_first = jax.random.randint(keys[3], (blocks, T_DEV), 1, EXPERTS)
    offset = jax.random.randint(keys[4], (blocks, T_DEV), 1, EXPERTS - 1)
    other_second = (other_first - 1 + offset) % (EXPERTS - 1) + 1
    first = jnp.where(chosen, 0, other_first)
    second = jnp.where(chosen, other_first, other_second)
    flipped = jax.random.randint(keys[5], (blocks, T_DEV), 0, 2) == 1
    left = jnp.where(flipped, second, first)
    right = jnp.where(flipped, first, second)
    return jnp.stack([left, right], axis=-1).reshape(TOKENS, 2).astype(jnp.int32)


def touch_ends(values, rng, smallest, top_value):
    spot = [jax.random.randint(jax.random.fold_in(rng, axis), (), 0, length) for axis, length in enumerate(values.shape)]
    main_axis = values.shape.index(max(values.shape))
    next_to = spot[:main_axis] + [(spot[main_axis] + 1) % values.shape[main_axis]] + spot[main_axis + 1:]
    return values.at[tuple(spot)].set(smallest).at[tuple(next_to)].set(top_value)


def steps_of(stream_key, dims, cuts, least, high):
    def one(dim, blocks):
        steps = jax.random.uniform(jax.random.fold_in(jax.random.fold_in(stream_key, 6), dim), (blocks,), jnp.float32, least / len(cuts), high / len(cuts))
        return jnp.repeat(jnp.exp(steps), dims[dim] // blocks).reshape((-1,) + (1,) * (len(dims) - dim - 1))

    gain = one(*cuts[0])
    for cut in cuts[1:]:
        gain = gain * one(*cut)
    return gain


def normal_values(own_key, shape, spread, most, cuts=(), held_as=jnp.bfloat16):
    drawn = spread * jax.random.normal(own_key, shape, jnp.float32)
    if cuts:
        drawn = drawn * steps_of(own_key, shape, cuts, -0.22, 0.18)
    return jnp.clip(drawn, -most, most).astype(held_as)


def setup_inputs(seed: int = 0) -> dict:
    streams_of = jax.random.split(jax.random.key(seed), 7)
    return {
        "tokens": normal_values(streams_of[0], (TOKENS, D), 1.0, 6.0, ((0, 32),)),
        "expert_ids": draw_expert_ids(jax.random.fold_in(streams_of[6], 71), 0),
        "gate_num": touch_ends(jax.random.randint(streams_of[2], (TOKENS,), 1, 256), jax.random.fold_in(streams_of[2], 1), 1, 255).astype(jnp.int32),
        "gate_weight": normal_values(streams_of[3], (D, FF), D ** -0.5, 0.109375, ((0, 4), (1, 8))),
        "up_weight": normal_values(streams_of[4], (D, FF), D ** -0.5, 0.109375, ((0, 4), (1, 8))),
        "down_weight": normal_values(streams_of[5], (FF, D), FF ** -0.5, 0.0625, ((0, 32),)),
    }


GATE_SCALE = 256.0


def route_table(expert_ids, slot_count):
    hits = jnp.sum((expert_ids == 0).astype(jnp.int32), axis=1)
    position = jnp.cumsum(hits) - 1
    marks = (hits[:, None] > 0) & (position[:, None] == jnp.arange(slot_count, dtype=jnp.int32)[None, :])
    return marks.astype(jnp.float32)


def gate_values(expert_ids, gate_num):
    first = gate_num.astype(jnp.float32) / GATE_SCALE
    return jnp.where(expert_ids[:, 0] == 0, first, 0.0) + jnp.where(expert_ids[:, 1] == 0, 1.0 - first, 0.0)


def reference(tokens, expert_ids, gate_num, gate_weight, up_weight, down_weight):
    slot_count = T_DEV // 2
    block_len = FF // N_BLK
    grouped_x = tokens.reshape(N_BLK, N_DP, T_DEV, D)
    grouped_ids = expert_ids.reshape(N_BLK, N_DP, T_DEV, 2)
    grouped_num = gate_num.reshape(N_BLK, N_DP, T_DEV)

    def one_group(inputs):
        block_x, block_ids, block_num = inputs
        marks = jax.vmap(lambda ids: route_table(ids, slot_count))(block_ids)
        packed = jnp.einsum("btc,btd->bcd", marks, block_x.astype(jnp.float32)).astype(jnp.bfloat16)
        packed = packed.reshape(N_DP * slot_count, D)
        gate = jnp.dot(packed, gate_weight, preferred_element_type=jnp.float32)
        up = jnp.dot(packed, up_weight, preferred_element_type=jnp.float32)
        hidden = (jax.nn.silu(gate) * up).astype(jnp.bfloat16)

        def add_block(running, index):
            start = (index * block_len).astype(jnp.int32)
            columns = lax.dynamic_slice_in_dim(hidden, start, block_len, 1)
            rows = lax.dynamic_slice_in_dim(down_weight, start, block_len, 0)
            term = jnp.dot(columns, rows, preferred_element_type=jnp.float32).astype(jnp.bfloat16)
            term = lax.optimization_barrier(term)
            return running + term.astype(jnp.float32), None

        rows_out, _ = lax.scan(add_block, jnp.zeros((N_DP * slot_count, D), jnp.float32), jnp.arange(N_BLK, dtype=jnp.int32))
        rows_out = rows_out.reshape(N_DP, slot_count, D)
        expanded = jnp.einsum("btc,bcd->btd", marks, rows_out, precision=lax.Precision.HIGHEST)
        weights = jax.vmap(gate_values)(block_ids, block_num)
        return (weights[:, :, None] * expanded).astype(jnp.bfloat16)

    result = lax.map(one_group, (grouped_x, grouped_ids, grouped_num))
    return result.reshape(TOKENS, D)
```

```python
import functools

import jax
import jax.numpy as jnp
from jax import lax
from jax.experimental import pallas as pl
from jax.experimental.pallas import tpu as pltpu
from jax.sharding import PartitionSpec as P

GATE_SCALE = 256.0
MESH = pl.DeviceIdType.MESH
F32 = jnp.float32
BF16 = jnp.bfloat16


def largest_tile(size, most):
    tile = most
    while size % tile:
        tile //= 2
    return tile


def kernel(nb, nd, rows_ch, cols_ch,
           tokens, ids, num, gate_w, up_w, down_w,
           slots_out, marks_out,
           x, gw, uw, dw, accg, accu, hidden, term, got1, part, got2,
           loc_sem, own_send, own_recv, y_send, y_recv, fwd_send, fwd_recv,
           z_send, z_recv, x_send, x_recv, p1_send, p1_recv, p2_send, p2_recv):
    k = lax.axis_index("blk")
    j = lax.axis_index("dp")
    na, nc = nb // 2, nd // 2
    a, b = k // 2, k % 2
    y, core = j // 2, j % 2
    t_dev, depth = tokens.shape
    slots = t_dev // 2
    gate_rows, ff = gate_w.shape
    down_rows = down_w.shape[0]
    n_ch = gate_rows // rows_ch
    nq = depth // cols_ch
    mate = (k, y * 2 + 1 - core)
    x_peer = (a * 2 + 1 - b, j)

    def y_chip(d):
        return lax.rem(y + d, nc)

    def z_chip(d):
        return lax.rem(a + d, na)

    def y_dev(d):
        return (k, y_chip(d) * 2 + core)

    def z_dev(d):
        return (z_chip(d) * 2 + b, j)

    def remote(src, dst, send, recv, device):
        return pltpu.make_async_remote_copy(
            src_ref=src, dst_ref=dst, send_sem=send, recv_sem=recv,
            device_id=device, device_id_type=MESH)

    def piece(p, shard):
        if p < 2 * n_ch:
            rows = pl.ds((p // 2) * rows_ch, rows_ch)
            src, dst = ((gate_w, gw), (up_w, uw))[p % 2]
            return src.at[rows, :], dst.at[shard, rows, :]
        q = p - 2 * n_ch
        return down_w.at[:, pl.ds(q * cols_ch, cols_ch)], dw.at[q, shard]

    pieces = 2 * n_ch + nq

    peers = [mate, x_peer] + [y_dev(d) for d in range(1, nc)] + [z_dev(d) for d in range(1, na)]
    barrier = pltpu.get_barrier_semaphore()
    for peer in peers:
        pl.semaphore_signal(barrier, inc=1, device_id=peer, device_id_type=MESH)
    local = []
    for p in range(pieces):
        src, dst = piece(p, j)
        local.append(pltpu.make_async_copy(src, dst, loc_sem.at[p]))
        local[-1].start()
    pl.semaphore_wait(barrier, len(peers))

    y_copies = []
    for p in range(pieces):
        src, dst = piece(p, j)
        for d in range(1, nc):
            y_copies.append(remote(src, dst, y_send.at[d - 1, p], y_recv.at[d - 1, p], y_dev(d)))
            y_copies[-1].start()

    hit0 = (ids[:, 0:1] == 0).astype(F32)
    hit1 = (ids[:, 1:2] == 0).astype(F32)
    hit = hit0 + hit1
    row = lax.broadcasted_iota(jnp.int32, (t_dev, t_dev), 0)
    col = lax.broadcasted_iota(jnp.int32, (t_dev, t_dev), 1)
    lower = (col <= row).astype(F32)
    place = jnp.dot(lower.astype(BF16), jnp.broadcast_to(hit, (t_dev, t_dev)).astype(BF16),
                    preferred_element_type=F32) - 1.0
    marks = jnp.where(place == col.astype(F32), 1.0, 0.0) * hit
    marks_out[...] = marks[:, :slots].astype(BF16)
    m0 = (marks * hit0).T[:slots]
    m1 = (marks * hit1).T[:slots]
    first = num[...].astype(F32) / GATE_SCALE
    weight = jnp.sum(m0 * first + m1 * (1.0 - first), axis=1, keepdims=True)
    packer = (m0 + m1).astype(BF16)

    def block(aa, bb):
        return pl.ds(pl.multiple_of((bb * na + aa) * slots, slots), slots)

    mine = block(a, b)
    for s in range(nd):
        columns = tokens[:, s * gate_rows:(s + 1) * gate_rows]
        x[s, mine, :] = jnp.dot(packer, columns, preferred_element_type=F32).astype(BF16)

    t_copies = []
    for d in range(1, na):
        t_copies.append(remote(x.at[:, mine, :], x.at[:, mine, :], z_send.at[d - 1], z_recv.at[d - 1], z_dev(d)))
        t_copies[-1].start()
    t_copies.append(remote(x.at[:, mine, :], x.at[:, mine, :], x_send.at[0], x_recv.at[0], x_peer))
    t_copies[-1].start()

    own_copies = []
    for p in range(pieces):
        src, dst = piece(p, j)
        own_copies.append(remote(src, dst, own_send.at[p], own_recv.at[p], mate))
        own_copies[-1].start()

    accg[...] = jnp.zeros_like(accg)
    accu[...] = jnp.zeros_like(accu)

    for d in range(1, na):
        came = block(lax.rem(a + na - d, na), b)
        remote(x.at[:, came, :], x.at[:, came, :], z_send.at[d - 1], z_recv.at[d - 1], z_dev(d)).wait_recv()
        t_copies.append(remote(x.at[:, came, :], x.at[:, came, :], x_send.at[d], x_recv.at[d], x_peer))
        t_copies[-1].start()
    for d in range(na):
        came = block(lax.rem(a + na - d, na), 1 - b)
        remote(x.at[:, came, :], x.at[:, came, :], x_send.at[d], x_recv.at[d], x_peer).wait_recv()

    tile = largest_tile(ff, 256)

    def add_rows(shard, c):
        r0 = c * rows_ch

        @pl.loop(0, ff // tile)
        def _(n):
            cols = pl.ds(pl.multiple_of(n * tile, tile), tile)
            left = x[shard, :, pl.ds(r0, rows_ch)]
            accg[:, cols] += jnp.dot(left, gw[shard, pl.ds(r0, rows_ch), cols], preferred_element_type=F32)
            accu[:, cols] += jnp.dot(left, uw[shard, pl.ds(r0, rows_ch), cols], preferred_element_type=F32)

    other = y * 2 + 1 - core
    for c in range(n_ch):
        local[2 * c].wait()
        local[2 * c + 1].wait()
        add_rows(j, c)
    for c in range(n_ch):
        for p in (2 * c, 2 * c + 1):
            own_copies[p].wait_recv()
        add_rows(other, c)

    fwd_copies = []

    def forward(p):
        for d in range(1, nc):
            came = lax.rem(y + nc - d, nc) * 2 + core
            src, dst = piece(p, came)
            remote(src, dst, y_send.at[d - 1, p], y_recv.at[d - 1, p], y_dev(d)).wait_recv()
            fwd_copies.append(remote(dst, dst, fwd_send.at[d - 1, p], fwd_recv.at[d - 1, p], mate))
            fwd_copies[-1].start()

    def take(p):
        for d in range(1, nc):
            came = lax.rem(y + nc - d, nc) * 2 + 1 - core
            src, dst = piece(p, came)
            remote(dst, dst, fwd_send.at[d - 1, p], fwd_recv.at[d - 1, p], mate).wait_recv()

    for c in range(n_ch):
        forward(2 * c)
        forward(2 * c + 1)
        for d in range(1, nc):
            add_rows(lax.rem(y + nc - d, nc) * 2 + core, c)
        take(2 * c)
        take(2 * c + 1)
        for d in range(1, nc):
            add_rows(lax.rem(y + nc - d, nc) * 2 + 1 - core, c)

    rows_all = nb * slots
    htile = largest_tile(rows_all, 64)

    @pl.loop(0, rows_all // htile)
    def _(i):
        rows = pl.ds(pl.multiple_of(i * htile, htile), htile)
        g = accg[rows, :]
        hidden[rows, :] = (g / (1.0 + jnp.exp(-g)) * accu[rows, :]).astype(BF16)

    half = na * slots
    mtile = largest_tile(rows_all, 256)
    sums = []

    def multiply(q):
        p = 2 * n_ch + q
        forward(p)
        local[p].wait()
        own_copies[p].wait_recv()
        take(p)

        @pl.loop(0, rows_all // mtile)
        def _(i):
            rows = pl.ds(pl.multiple_of(i * mtile, mtile), mtile)
            term[q, rows, :] = jnp.dot(
                hidden[rows, :], dw[q].reshape(nd * down_rows, cols_ch),
                preferred_element_type=F32).astype(BF16)

        away = pl.ds(pl.multiple_of((1 - b) * half, half), half)
        sums.append(remote(term.at[q, away, :], got1.at[q], p1_send.at[q], p1_recv.at[q], x_peer))
        sums[-1].start()

    def pair(q):
        remote(got1.at[q], got1.at[q], p1_send.at[q], p1_recv.at[q], x_peer).wait_recv()
        here = pl.ds(pl.multiple_of(b * half, half), half)
        part[q] = (term[q, here, :].astype(F32) + got1[q].astype(F32)).astype(BF16)
        for d in range(1, na):
            rows = pl.ds(pl.multiple_of(z_chip(d) * slots, slots), slots)
            sums.append(remote(part.at[q, rows, :], got2.at[q, d - 1],
                               p2_send.at[q, d - 1], p2_recv.at[q, d - 1], z_dev(d)))
            sums[-1].start()

    def finish(q):
        for d in range(1, na):
            remote(got2.at[q, d - 1], got2.at[q, d - 1],
                   p2_send.at[q, d - 1], p2_recv.at[q, d - 1], z_dev(d)).wait_recv()
        total = part[q, pl.ds(pl.multiple_of(a * slots, slots), slots), :].astype(F32)
        for d in range(1, na):
            total += got2[q, d - 1].astype(F32)
        slots_out[:, pl.ds(q * cols_ch, cols_ch)] = (weight * total).astype(BF16)

    for q in range(nq + 2):
        if q < nq:
            multiply(q)
        if 1 <= q <= nq:
            pair(q - 1)
        if q >= 2:
            finish(q - 2)

    for copy in y_copies + t_copies + own_copies + fwd_copies + sums:
        copy.wait_send()


def on_device(nb, nd, tokens, expert_ids, gate_num, gate_weight, up_weight, down_weight):
    t_dev, depth = tokens.shape
    slots = t_dev // 2
    gate_rows, ff = gate_weight.shape
    down_rows = down_weight.shape[0]
    rows_ch = largest_tile(gate_rows, 256)
    if rows_ch % 128:
        rows_ch = gate_rows
    cols_ch = largest_tile(depth, 512)
    n_ch, nq = gate_rows // rows_ch, depth // cols_ch
    pieces = 2 * n_ch + nq
    na, nc = nb // 2, nd // 2
    rows_all = nb * slots
    dma = pltpu.SemaphoreType.DMA
    vmem = pl.BlockSpec(memory_space=pltpu.VMEM)
    hbm = pl.BlockSpec(memory_space=pl.ANY)
    far, deep = max(nc - 1, 1), max(na - 1, 1)
    packed, marks = pl.pallas_call(
        functools.partial(kernel, nb, nd, rows_ch, cols_ch),
        out_shape=(jax.ShapeDtypeStruct((slots, depth), BF16),
                   jax.ShapeDtypeStruct((t_dev, slots), BF16)),
        in_specs=[vmem, vmem, vmem, hbm, hbm, hbm],
        out_specs=(vmem, vmem),
        scratch_shapes=[
            pltpu.VMEM((nd, rows_all, gate_rows), BF16),
            pltpu.VMEM((nd, gate_rows, ff), BF16),
            pltpu.VMEM((nd, gate_rows, ff), BF16),
            pltpu.VMEM((nq, nd, down_rows, cols_ch), BF16),
            pltpu.VMEM((rows_all, ff), F32),
            pltpu.VMEM((rows_all, ff), F32),
            pltpu.VMEM((rows_all, ff), BF16),
            pltpu.VMEM((nq, rows_all, cols_ch), BF16),
            pltpu.VMEM((nq, na * slots, cols_ch), BF16),
            pltpu.VMEM((nq, na * slots, cols_ch), BF16),
            pltpu.VMEM((nq, deep, slots, cols_ch), BF16),
            dma((pieces,)), dma((pieces,)), dma((pieces,)),
            dma((far, pieces)), dma((far, pieces)), dma((far, pieces)), dma((far, pieces)),
            dma((deep,)), dma((deep,)), dma((na,)), dma((na,)),
            dma((nq,)), dma((nq,)), dma((nq, deep)), dma((nq, deep)),
        ],
        compiler_params=pltpu.CompilerParams(
            collective_id=0, has_side_effects=True, vmem_limit_bytes=60 * 1024 * 1024),
    )(tokens, expert_ids, gate_num.reshape(1, t_dev), gate_weight, up_weight, down_weight)
    return jnp.dot(marks, packed, preferred_element_type=F32).astype(BF16)


def solution(mesh):
    return jax.shard_map(
        functools.partial(on_device, mesh.shape["blk"], mesh.shape["dp"]),
        mesh=mesh,
        in_specs=(
            P(("blk", "dp"), None),
            P(("blk", "dp"), None),
            P(("blk", "dp")),
            P("dp", "blk"),
            P("dp", "blk"),
            P(("blk", "dp"), None),
        ),
        out_specs=P(("blk", "dp"), None),
        check_vma=False,
    )
```

```python
import functools

import jax
import jax.numpy as jnp
from jax import lax
from jax.experimental import pallas as pl
from jax.experimental.pallas import tpu as pltpu
from jax.sharding import PartitionSpec as P

GATE_SCALE = 256.0
MESH = pl.DeviceIdType.MESH
F32 = jnp.float32
BF16 = jnp.bfloat16


def largest_tile(size, most):
    tile = most
    while size % tile:
        tile //= 2
    return tile


def kernel(nb, nd, cols_ch,
           tokens, ids, num, gate_w, up_w, down_w,
           slots_out, marks_out,
           x, packed, gw, uw, dw, accg, accu, away, back, hidden, term, got1, part, got2,
           loc_sem, own_send, own_recv, y_send, y_recv, fwd_send, fwd_recv,
           t_send, t_recv, s_send, s_recv,
           z_send, z_recv, x_send, x_recv, p1_send, p1_recv, p2_send, p2_recv):
    k = lax.axis_index("blk")
    j = lax.axis_index("dp")
    na, nc = nb // 2, nd // 2
    a, b = k // 2, k % 2
    y, core = j // 2, j % 2
    t_dev, depth = tokens.shape
    slots = t_dev // 2
    gate_rows, ff = gate_w.shape
    down_rows = down_w.shape[0]
    width = 2 * gate_rows
    nq = depth // cols_ch
    mate = (k, y * 2 + 1 - core)
    x_peer = (a * 2 + 1 - b, j)

    def y_dev(d):
        return (k, lax.rem(y + d, nc) * 2 + core)

    def z_chip(d):
        return lax.rem(a + d, na)

    def z_dev(d):
        return (z_chip(d) * 2 + b, j)

    def remote(src, dst, send, recv, device):
        return pltpu.make_async_remote_copy(
            src_ref=src, dst_ref=dst, send_sem=send, recv_sem=recv,
            device_id=device, device_id_type=MESH)

    def block(aa, bb):
        return bb * na + aa

    def block_rows(aa, bb):
        return pl.ds(pl.multiple_of(block(aa, bb) * slots, slots), slots)

    def piece(p, core_of, shard):
        if p < 2:
            rows = pl.ds(pl.multiple_of(core_of * gate_rows, 16), gate_rows)
            src, dst = ((gate_w, gw), (up_w, uw))[p]
            return src, dst.at[rows, :]
        q = p - 2
        return down_w.at[:, pl.ds(q * cols_ch, cols_ch)], dw.at[q, shard]

    pieces = 2 + nq

    peers = [mate, x_peer] + [y_dev(d) for d in range(1, nc)] + [z_dev(d) for d in range(1, na)]
    barrier = pltpu.get_barrier_semaphore()
    for peer in peers:
        pl.semaphore_signal(barrier, inc=1, device_id=peer, device_id_type=MESH)
    local = []
    for p in range(pieces):
        src, dst = piece(p, core, j)
        local.append(pltpu.make_async_copy(src, dst, loc_sem.at[p]))
        local[-1].start()

    hit0 = (ids[:, 0:1] == 0).astype(F32)
    hit1 = (ids[:, 1:2] == 0).astype(F32)
    hit = hit0 + hit1
    row = lax.broadcasted_iota(jnp.int32, (t_dev, t_dev), 0)
    col = lax.broadcasted_iota(jnp.int32, (t_dev, t_dev), 1)
    lower = (col <= row).astype(F32)
    place = jnp.dot(lower.astype(BF16), jnp.broadcast_to(hit, (t_dev, t_dev)).astype(BF16),
                    preferred_element_type=F32) - 1.0
    marks = jnp.where(place == col.astype(F32), 1.0, 0.0) * hit
    marks_out[...] = marks[:, :slots].astype(BF16)
    m0 = (marks * hit0).T[:slots]
    m1 = (marks * hit1).T[:slots]
    first = num[...].astype(F32) / GATE_SCALE
    weight = jnp.sum(m0 * first + m1 * (1.0 - first), axis=1, keepdims=True)
    packer = (m0 + m1).astype(BF16)

    def pack(d):
        columns = pl.ds(pl.multiple_of(lax.rem(y + d, nc) * width, 128), width)
        return jnp.dot(packer, tokens[:, columns], preferred_element_type=F32).astype(BF16)

    mine = block(a, b)
    for d in range(1, nc):
        packed[d - 1] = pack(d)
    x[mine, 0] = pack(0)

    pl.semaphore_wait(barrier, len(peers))

    copies = []

    def send(*args):
        copies.append(remote(*args))
        copies[-1].start()

    for d in range(1, nc):
        send(packed.at[d - 1], x.at[mine, nc - d], t_send.at[d - 1], t_recv.at[d - 1], y_dev(d))
    for p in range(2):
        src, dst = piece(p, core, j)
        send(src, dst, own_send.at[p], own_recv.at[p], mate)

    def send_down(q):
        src, dst = piece(2 + q, core, j)
        for d in range(1, nc):
            send(src, dst, y_send.at[d - 1, q], y_recv.at[d - 1, q], y_dev(d))

    early = min(1, nq)
    for q in range(early):
        send_down(q)
    send(x.at[mine, 0], x.at[mine, 0], x_send.at[0], x_recv.at[0], x_peer)
    for d in range(1, na):
        send(x.at[mine, 0], x.at[mine, 0], z_send.at[0, d - 1], z_recv.at[0, d - 1], z_dev(d))
    for d in range(1, nc):
        remote(packed.at[d - 1], x.at[mine, nc - d], t_send.at[d - 1], t_recv.at[d - 1], y_dev(d)).wait_recv()
    rest = x.at[mine, pl.ds(1, nc - 1)]
    send(rest, rest, x_send.at[na], x_recv.at[na], x_peer)
    for d in range(1, na):
        send(rest, rest, z_send.at[1, d - 1], z_recv.at[1, d - 1], z_dev(d))
    for p in range(2, pieces):
        src, dst = piece(p, core, j)
        send(src, dst, own_send.at[p], own_recv.at[p], mate)

    for p in range(2):
        local[p].wait()
        src, dst = piece(p, 1 - core, j)
        remote(src, dst, own_send.at[p], own_recv.at[p], mate).wait_recv()

    tile = largest_tile(ff, 256)

    def multiply_block(i, aa, bb):
        which = block(aa, bb)
        rows = block_rows(aa, bb)

        @pl.loop(0, ff // tile)
        def _(n):
            c0 = pl.multiple_of(n * tile, tile)
            cols = pl.ds(c0, tile)
            left = x[which].reshape(nc * slots, width)
            for w, acc, start in ((gw, accg, 0), (uw, accu, ff)):
                value = jnp.dot(left, w[:, cols], preferred_element_type=F32)
                acc[rows, cols] = value[:slots]
                for d in range(1, nc):
                    away[i, d - 1, :, pl.ds(pl.multiple_of(start + c0, tile), tile)] = (
                        value[d * slots:(d + 1) * slots].astype(BF16))

        for d in range(1, nc):
            send(away.at[i, d - 1], back.at[i, d - 1], s_send.at[i, d - 1], s_recv.at[i, d - 1], y_dev(d))

    def activate(i, aa, bb):
        rows = block_rows(aa, bb)
        for d in range(1, nc):
            remote(away.at[i, d - 1], back.at[i, d - 1], s_send.at[i, d - 1], s_recv.at[i, d - 1], y_dev(d)).wait_recv()

        @pl.loop(0, ff // tile)
        def _(n):
            c0 = pl.multiple_of(n * tile, tile)
            cols = pl.ds(c0, tile)
            g = accg[rows, cols]
            u = accu[rows, cols]
            for d in range(1, nc):
                g += back[i, d - 1, :, cols].astype(F32)
                u += back[i, d - 1, :, pl.ds(pl.multiple_of(ff + c0, tile), tile)].astype(F32)
            hidden[rows, cols] = (g / (1.0 + jnp.exp(-g)) * u).astype(BF16)

    order = []
    for d in range(na):
        source = lax.rem(a + na - d, na)
        order += [(source, b), (source, 1 - b)]
    lag = 2
    for i in range(nb + lag):
        if i < nb:
            d = i // 2
            aa, bb = order[i]
            here = x.at[block(aa, bb)]
            if i == 1:
                first_part = here.at[0]
                other_part = here.at[pl.ds(1, nc - 1)]
                remote(first_part, first_part, x_send.at[0], x_recv.at[0], x_peer).wait_recv()
                remote(other_part, other_part, x_send.at[na], x_recv.at[na], x_peer).wait_recv()
            elif i % 2:
                remote(here, here, x_send.at[d], x_recv.at[d], x_peer).wait_recv()
            elif i:
                first_part = here.at[0]
                other_part = here.at[pl.ds(1, nc - 1)]
                remote(first_part, first_part, z_send.at[0, d - 1], z_recv.at[0, d - 1], z_dev(d)).wait_recv()
                remote(other_part, other_part, z_send.at[1, d - 1], z_recv.at[1, d - 1], z_dev(d)).wait_recv()
                send(here, here, x_send.at[d], x_recv.at[d], x_peer)
            multiply_block(i, aa, bb)
            if i == nb - 1:
                for q in range(early, nq):
                    send_down(q)
        if i >= lag:
            activate(i - lag, *order[i - lag])

    rows_all = nb * slots
    half = na * slots
    mtile = largest_tile(rows_all, 256)

    def multiply(q):
        for d in range(1, nc):
            came = dw.at[q, lax.rem(y + nc - d, nc) * 2 + core]
            remote(came, came, y_send.at[d - 1, q], y_recv.at[d - 1, q], y_dev(d)).wait_recv()
            send(came, came, fwd_send.at[d - 1, q], fwd_recv.at[d - 1, q], mate)
        local[2 + q].wait()
        theirs = dw.at[q, y * 2 + 1 - core]
        remote(theirs, theirs, own_send.at[2 + q], own_recv.at[2 + q], mate).wait_recv()
        for d in range(1, nc):
            came = dw.at[q, lax.rem(y + nc - d, nc) * 2 + 1 - core]
            remote(came, came, fwd_send.at[d - 1, q], fwd_recv.at[d - 1, q], mate).wait_recv()

        @pl.loop(0, rows_all // mtile)
        def _(i):
            rows = pl.ds(pl.multiple_of(i * mtile, mtile), mtile)
            term[q, rows, :] = jnp.dot(
                hidden[rows, :], dw[q].reshape(nd * down_rows, cols_ch),
                preferred_element_type=F32).astype(BF16)

        other = pl.ds(pl.multiple_of((1 - b) * half, half), half)
        send(term.at[q, other, :], got1.at[q], p1_send.at[q], p1_recv.at[q], x_peer)

    def pair(q):
        remote(got1.at[q], got1.at[q], p1_send.at[q], p1_recv.at[q], x_peer).wait_recv()
        here = pl.ds(pl.multiple_of(b * half, half), half)
        part[q] = (term[q, here, :].astype(F32) + got1[q].astype(F32)).astype(BF16)
        for d in range(1, na):
            rows = pl.ds(pl.multiple_of(z_chip(d) * slots, slots), slots)
            send(part.at[q, rows, :], got2.at[q, d - 1],
                 p2_send.at[q, d - 1], p2_recv.at[q, d - 1], z_dev(d))

    def finish(q):
        for d in range(1, na):
            remote(got2.at[q, d - 1], got2.at[q, d - 1],
                   p2_send.at[q, d - 1], p2_recv.at[q, d - 1], z_dev(d)).wait_recv()
        total = part[q, pl.ds(pl.multiple_of(a * slots, slots), slots), :].astype(F32)
        for d in range(1, na):
            total += got2[q, d - 1].astype(F32)
        slots_out[:, pl.ds(q * cols_ch, cols_ch)] = (weight * total).astype(BF16)

    for q in range(nq + 2):
        if q < nq:
            multiply(q)
        if 1 <= q <= nq:
            pair(q - 1)
        if q >= 2:
            finish(q - 2)

    for copy in copies:
        copy.wait_send()


def on_device(nb, nd, tokens, expert_ids, gate_num, gate_weight, up_weight, down_weight):
    t_dev, depth = tokens.shape
    slots = t_dev // 2
    gate_rows, ff = gate_weight.shape
    down_rows = down_weight.shape[0]
    cols_ch = largest_tile(depth, 256)
    nq = depth // cols_ch
    pieces = 2 + nq
    na, nc = nb // 2, nd // 2
    rows_all = nb * slots
    dma = pltpu.SemaphoreType.DMA
    vmem = pl.BlockSpec(memory_space=pltpu.VMEM)
    hbm = pl.BlockSpec(memory_space=pl.ANY)
    far, deep = max(nc - 1, 1), max(na - 1, 1)
    packed, marks = pl.pallas_call(
        functools.partial(kernel, nb, nd, cols_ch),
        out_shape=(jax.ShapeDtypeStruct((slots, depth), BF16),
                   jax.ShapeDtypeStruct((t_dev, slots), BF16)),
        in_specs=[vmem, vmem, vmem, hbm, hbm, hbm],
        out_specs=(vmem, vmem),
        scratch_shapes=[
            pltpu.VMEM((nb, nc, slots, 2 * gate_rows), BF16),
            pltpu.VMEM((far, slots, 2 * gate_rows), BF16),
            pltpu.VMEM((2 * gate_rows, ff), BF16),
            pltpu.VMEM((2 * gate_rows, ff), BF16),
            pltpu.VMEM((nq, nd, down_rows, cols_ch), BF16),
            pltpu.VMEM((rows_all, ff), F32),
            pltpu.VMEM((rows_all, ff), F32),
            pltpu.VMEM((nb, far, slots, 2 * ff), BF16),
            pltpu.VMEM((nb, far, slots, 2 * ff), BF16),
            pltpu.VMEM((rows_all, ff), BF16),
            pltpu.VMEM((nq, rows_all, cols_ch), BF16),
            pltpu.VMEM((nq, na * slots, cols_ch), BF16),
            pltpu.VMEM((nq, na * slots, cols_ch), BF16),
            pltpu.VMEM((nq, deep, slots, cols_ch), BF16),
            dma((pieces,)), dma((pieces,)), dma((pieces,)),
            dma((far, nq)), dma((far, nq)), dma((far, nq)), dma((far, nq)),
            dma((far,)), dma((far,)), dma((nb, far)), dma((nb, far)),
            dma((2, deep)), dma((2, deep)), dma((na + 1,)), dma((na + 1,)),
            dma((nq,)), dma((nq,)), dma((nq, deep)), dma((nq, deep)),
        ],
        compiler_params=pltpu.CompilerParams(
            collective_id=0, has_side_effects=True, vmem_limit_bytes=67043328),
    )(tokens, expert_ids, gate_num.reshape(1, t_dev), gate_weight, up_weight, down_weight)
    return jnp.dot(marks, packed, preferred_element_type=F32).astype(BF16)


def solution(mesh):
    return jax.shard_map(
        functools.partial(on_device, mesh.shape["blk"], mesh.shape["dp"]),
        mesh=mesh,
        in_specs=(
            P(("blk", "dp"), None),
            P(("blk", "dp"), None),
            P(("blk", "dp")),
            P("dp", "blk"),
            P("dp", "blk"),
            P(("blk", "dp"), None),
        ),
        out_specs=P(("blk", "dp"), None),
        check_vma=False,
    )
```

```python
import functools

import jax
import jax.numpy as jnp
from jax import lax
from jax.experimental import pallas as pl
from jax.experimental.pallas import tpu as pltpu
from jax.sharding import PartitionSpec as P

GATE_SCALE = 256.0
MESH = pl.DeviceIdType.MESH
F32 = jnp.float32
BF16 = jnp.bfloat16


def largest_tile(size, most):
    tile = most
    while size % tile:
        tile //= 2
    return tile


def kernel(nb, nd, rows_ch, cols_ch,
           tokens, ids, num, gate_w, up_w, down_w,
           slots_out, marks_out,
           x, gw, uw, dw, accg, accu, hidden, term, got1, part, got2,
           loc_sem, own_send, own_recv, y_send, y_recv, fwd_send, fwd_recv,
           z_send, z_recv, x_send, x_recv, p1_send, p1_recv, p2_send, p2_recv):
    k = lax.axis_index("blk")
    j = lax.axis_index("dp")
    na, nc = nb // 2, nd // 2
    a, b = k // 2, k % 2
    y, core = j // 2, j % 2
    t_dev, depth = tokens.shape
    slots = t_dev // 2
    gate_rows, ff = gate_w.shape
    down_rows = down_w.shape[0]
    n_ch = gate_rows // rows_ch
    nq = depth // cols_ch
    mate = (k, y * 2 + 1 - core)
    x_peer = (a * 2 + 1 - b, j)

    def y_chip(d):
        return lax.rem(y + d, nc)

    def z_chip(d):
        return lax.rem(a + d, na)

    def y_dev(d):
        return (k, y_chip(d) * 2 + core)

    def z_dev(d):
        return (z_chip(d) * 2 + b, j)

    def remote(src, dst, send, recv, device):
        return pltpu.make_async_remote_copy(
            src_ref=src, dst_ref=dst, send_sem=send, recv_sem=recv,
            device_id=device, device_id_type=MESH)

    def piece(p, shard):
        if p < 2 * n_ch:
            rows = pl.ds((p // 2) * rows_ch, rows_ch)
            src, dst = ((gate_w, gw), (up_w, uw))[p % 2]
            return src.at[rows, :], dst.at[shard, rows, :]
        q = p - 2 * n_ch
        return down_w.at[:, pl.ds(q * cols_ch, cols_ch)], dw.at[q, shard]

    pieces = 2 * n_ch + nq

    peers = [mate, x_peer] + [y_dev(d) for d in range(1, nc)] + [z_dev(d) for d in range(1, na)]
    barrier = pltpu.get_barrier_semaphore()
    for peer in peers:
        pl.semaphore_signal(barrier, inc=1, device_id=peer, device_id_type=MESH)
    local = []
    for p in range(pieces):
        src, dst = piece(p, j)
        local.append(pltpu.make_async_copy(src, dst, loc_sem.at[p]))
        local[-1].start()
    pl.semaphore_wait(barrier, len(peers))

    y_copies = []
    for p in range(pieces):
        src, dst = piece(p, j)
        for d in range(1, nc):
            y_copies.append(remote(src, dst, y_send.at[d - 1, p], y_recv.at[d - 1, p], y_dev(d)))
            y_copies[-1].start()

    hit0 = (ids[:, 0:1] == 0).astype(F32)
    hit1 = (ids[:, 1:2] == 0).astype(F32)
    hit = hit0 + hit1
    row = lax.broadcasted_iota(jnp.int32, (t_dev, t_dev), 0)
    col = lax.broadcasted_iota(jnp.int32, (t_dev, t_dev), 1)
    lower = (col <= row).astype(F32)
    place = jnp.dot(lower.astype(BF16), jnp.broadcast_to(hit, (t_dev, t_dev)).astype(BF16),
                    preferred_element_type=F32) - 1.0
    marks = jnp.where(place == col.astype(F32), 1.0, 0.0) * hit
    marks_out[...] = marks[:, :slots].astype(BF16)
    m0 = (marks * hit0).T[:slots]
    m1 = (marks * hit1).T[:slots]
    first = num[...].astype(F32) / GATE_SCALE
    weight = jnp.sum(m0 * first + m1 * (1.0 - first), axis=1, keepdims=True)
    packer = (m0 + m1).astype(BF16)

    def block(aa, bb):
        return pl.ds(pl.multiple_of((bb * na + aa) * slots, slots), slots)

    mine = block(a, b)
    for s in range(nd):
        columns = tokens[:, s * gate_rows:(s + 1) * gate_rows]
        x[s, mine, :] = jnp.dot(packer, columns, preferred_element_type=F32).astype(BF16)

    t_copies = []
    for d in range(1, na):
        t_copies.append(remote(x.at[:, mine, :], x.at[:, mine, :], z_send.at[d - 1], z_recv.at[d - 1], z_dev(d)))
        t_copies[-1].start()
    t_copies.append(remote(x.at[:, mine, :], x.at[:, mine, :], x_send.at[0], x_recv.at[0], x_peer))
    t_copies[-1].start()

    own_copies = []
    for p in range(pieces):
        src, dst = piece(p, j)
        own_copies.append(remote(src, dst, own_send.at[p], own_recv.at[p], mate))
        own_copies[-1].start()

    accg[...] = jnp.zeros_like(accg)
    accu[...] = jnp.zeros_like(accu)

    for d in range(1, na):
        came = block(lax.rem(a + na - d, na), b)
        remote(x.at[:, came, :], x.at[:, came, :], z_send.at[d - 1], z_recv.at[d - 1], z_dev(d)).wait_recv()
        t_copies.append(remote(x.at[:, came, :], x.at[:, came, :], x_send.at[d], x_recv.at[d], x_peer))
        t_copies[-1].start()
    for d in range(na):
        came = block(lax.rem(a + na - d, na), 1 - b)
        remote(x.at[:, came, :], x.at[:, came, :], x_send.at[d], x_recv.at[d], x_peer).wait_recv()

    tile = largest_tile(ff, 256)

    def add_rows(shard, c):
        r0 = c * rows_ch

        @pl.loop(0, ff // tile)
        def _(n):
            cols = pl.ds(pl.multiple_of(n * tile, tile), tile)
            left = x[shard, :, pl.ds(r0, rows_ch)]
            accg[:, cols] += jnp.dot(left, gw[shard, pl.ds(r0, rows_ch), cols], preferred_element_type=F32)
            accu[:, cols] += jnp.dot(left, uw[shard, pl.ds(r0, rows_ch), cols], preferred_element_type=F32)

    other = y * 2 + 1 - core
    for c in range(n_ch):
        local[2 * c].wait()
        local[2 * c + 1].wait()
        add_rows(j, c)
    for c in range(n_ch):
        for p in (2 * c, 2 * c + 1):
            own_copies[p].wait_recv()
        add_rows(other, c)

    fwd_copies = []

    def forward(p):
        for d in range(1, nc):
            came = lax.rem(y + nc - d, nc) * 2 + core
            src, dst = piece(p, came)
            remote(src, dst, y_send.at[d - 1, p], y_recv.at[d - 1, p], y_dev(d)).wait_recv()
            fwd_copies.append(remote(dst, dst, fwd_send.at[d - 1, p], fwd_recv.at[d - 1, p], mate))
            fwd_copies[-1].start()

    def take(p):
        for d in range(1, nc):
            came = lax.rem(y + nc - d, nc) * 2 + 1 - core
            src, dst = piece(p, came)
            remote(dst, dst, fwd_send.at[d - 1, p], fwd_recv.at[d - 1, p], mate).wait_recv()

    for c in range(n_ch):
        forward(2 * c)
        forward(2 * c + 1)
        for d in range(1, nc):
            add_rows(lax.rem(y + nc - d, nc) * 2 + core, c)
        take(2 * c)
        take(2 * c + 1)
        for d in range(1, nc):
            add_rows(lax.rem(y + nc - d, nc) * 2 + 1 - core, c)

    rows_all = nb * slots
    htile = largest_tile(rows_all, 64)

    @pl.loop(0, rows_all // htile)
    def _(i):
        rows = pl.ds(pl.multiple_of(i * htile, htile), htile)
        g = accg[rows, :]
        hidden[rows, :] = (g / (1.0 + jnp.exp(-g)) * accu[rows, :]).astype(BF16)

    half = na * slots
    mtile = largest_tile(rows_all, 256)
    sums = []

    def multiply(q):
        p = 2 * n_ch + q
        forward(p)
        local[p].wait()
        own_copies[p].wait_recv()
        take(p)

        @pl.loop(0, rows_all // mtile)
        def _(i):
            rows = pl.ds(pl.multiple_of(i * mtile, mtile), mtile)
            term[q, rows, :] = jnp.dot(
                hidden[rows, :], dw[q].reshape(nd * down_rows, cols_ch),
                preferred_element_type=F32).astype(BF16)

        away = pl.ds(pl.multiple_of((1 - b) * half, half), half)
        sums.append(remote(term.at[q, away, :], got1.at[q], p1_send.at[q], p1_recv.at[q], x_peer))
        sums[-1].start()

    def pair(q):
        remote(got1.at[q], got1.at[q], p1_send.at[q], p1_recv.at[q], x_peer).wait_recv()
        here = pl.ds(pl.multiple_of(b * half, half), half)
        part[q] = (term[q, here, :].astype(F32) + got1[q].astype(F32)).astype(BF16)
        for d in range(1, na):
            rows = pl.ds(pl.multiple_of(z_chip(d) * slots, slots), slots)
            sums.append(remote(part.at[q, rows, :], got2.at[q, d - 1],
                               p2_send.at[q, d - 1], p2_recv.at[q, d - 1], z_dev(d)))
            sums[-1].start()

    def finish(q):
        for d in range(1, na):
            remote(got2.at[q, d - 1], got2.at[q, d - 1],
                   p2_send.at[q, d - 1], p2_recv.at[q, d - 1], z_dev(d)).wait_recv()
        total = part[q, pl.ds(pl.multiple_of(a * slots, slots), slots), :].astype(F32)
        for d in range(1, na):
            total += got2[q, d - 1].astype(F32)
        slots_out[:, pl.ds(q * cols_ch, cols_ch)] = (weight * total).astype(BF16)

    for q in range(nq + 2):
        if q < nq:
            multiply(q)
        if 1 <= q <= nq:
            pair(q - 1)
        if q >= 2:
            finish(q - 2)

    for copy in y_copies + t_copies + own_copies + fwd_copies + sums:
        copy.wait_send()


def on_device(nb, nd, tokens, expert_ids, gate_num, gate_weight, up_weight, down_weight):
    t_dev, depth = tokens.shape
    slots = t_dev // 2
    gate_rows, ff = gate_weight.shape
    down_rows = down_weight.shape[0]
    rows_ch = largest_tile(gate_rows, 256)
    if rows_ch % 128:
        rows_ch = gate_rows
    cols_ch = largest_tile(depth, 256)
    n_ch, nq = gate_rows // rows_ch, depth // cols_ch
    pieces = 2 * n_ch + nq
    na, nc = nb // 2, nd // 2
    rows_all = nb * slots
    dma = pltpu.SemaphoreType.DMA
    vmem = pl.BlockSpec(memory_space=pltpu.VMEM)
    hbm = pl.BlockSpec(memory_space=pl.ANY)
    far, deep = max(nc - 1, 1), max(na - 1, 1)
    packed, marks = pl.pallas_call(
        functools.partial(kernel, nb, nd, rows_ch, cols_ch),
        out_shape=(jax.ShapeDtypeStruct((slots, depth), BF16),
                   jax.ShapeDtypeStruct((t_dev, slots), BF16)),
        in_specs=[vmem, vmem, vmem, hbm, hbm, hbm],
        out_specs=(vmem, vmem),
        scratch_shapes=[
            pltpu.VMEM((nd, rows_all, gate_rows), BF16),
            pltpu.VMEM((nd, gate_rows, ff), BF16),
            pltpu.VMEM((nd, gate_rows, ff), BF16),
            pltpu.VMEM((nq, nd, down_rows, cols_ch), BF16),
            pltpu.VMEM((rows_all, ff), F32),
            pltpu.VMEM((rows_all, ff), F32),
            pltpu.VMEM((rows_all, ff), BF16),
            pltpu.VMEM((nq, rows_all, cols_ch), BF16),
            pltpu.VMEM((nq, na * slots, cols_ch), BF16),
            pltpu.VMEM((nq, na * slots, cols_ch), BF16),
            pltpu.VMEM((nq, deep, slots, cols_ch), BF16),
            dma((pieces,)), dma((pieces,)), dma((pieces,)),
            dma((far, pieces)), dma((far, pieces)), dma((far, pieces)), dma((far, pieces)),
            dma((deep,)), dma((deep,)), dma((na,)), dma((na,)),
            dma((nq,)), dma((nq,)), dma((nq, deep)), dma((nq, deep)),
        ],
        compiler_params=pltpu.CompilerParams(
            collective_id=0, has_side_effects=True, vmem_limit_bytes=60 * 1024 * 1024),
    )(tokens, expert_ids, gate_num.reshape(1, t_dev), gate_weight, up_weight, down_weight)
    return jnp.dot(marks, packed, preferred_element_type=F32).astype(BF16)


def solution(mesh):
    return jax.shard_map(
        functools.partial(on_device, mesh.shape["blk"], mesh.shape["dp"]),
        mesh=mesh,
        in_specs=(
            P(("blk", "dp"), None),
            P(("blk", "dp"), None),
            P(("blk", "dp")),
            P("dp", "blk"),
            P("dp", "blk"),
            P(("blk", "dp"), None),
        ),
        out_specs=P(("blk", "dp"), None),
        check_vma=False,
    )
```
